32 devices in a mesh: dp: 1, vocab: 32 (over z, y, x, core).
Axes of the slice: x: 2, y: 2, z: 4, core: 2. Of those that a mesh axis runs over, the one named last changes fastest.
Arguments:
- input_ids: int32 [256], P('dp'), may hold values from 0 to 63999
- target_ids: int32 [256], P('dp'), may hold values from 0 to 63999
- loss_mask: int32 [256], P('dp'), may hold values 0 or 1
- final_hidden: bfloat16 [256, 3584], P('dp'), may hold values from -5 to 5, as said below
- norm_gain: float32 [3584], replicated, may hold values from 0.25 to 1.75
- embed_cotangent: bfloat16 [256, 3584], P('dp'), may hold values from -0.059814453 to 0.059814453
- table: bfloat16 [64000, 3584], P(('dp', 'vocab')), may hold values from -0.08351914 to 0.08351914, as said below
Outputs:
- embedded: bfloat16 [256, 3584], P('dp')
- loss: float32 [], replicated
- grad_hidden: bfloat16 [256, 3584], P('dp')
- gain_grad: float32 [3584], replicated
- table_grad: bfloat16 [64000, 3584], P(('dp', 'vocab'))
The draws below stay inside these ranges and needn't reach their ends.
Inputs may be any that keep to these rules, and one draw needn't show every extreme that they name: Every entry of table lies within -5 / sqrt(3584) and 5 / sqrt(3584). Every entry of final_hidden lies within -5 and 5.
All inputs are finite; a program needn't handle non-finite values.
Results may differ from the reference program's by a relative error of at most 0.003.
Values may be sent and summed in bfloat16 or wider, within the bound.
A program may use at most 256 MiB of HBM per device.

```python
import math
import jax
import jax.numpy as jnp
import numpy as np
from jax import lax

D = 3584
SOFTCAP = 30
ROWS = 2000
V = 64000
TOKENS = 256
N_DP = 1
N_VOCAB = 32


def hub_layout(key):
    hub_stride = ROWS // 4
    hub_count = V // hub_stride
    unit_scale = 1.0 / math.sqrt(D)
    directions = jax.random.truncated_normal(jax.random.fold_in(key, 701), -4.0, 4.0, (hub_count, D), jnp.float32) * unit_scale
    return (hub_stride, hub_count, directions)


def draw_table(key, part):
    hub_stride, hub_count, directions = hub_layout(key)
    unit_scale = 1.0 / math.sqrt(D)
    noise_rows = jax.random.truncated_normal(jax.random.fold_in(key, 703), -4.0, 4.0, (V, D), jnp.float32)
    blocks = (noise_rows * unit_scale).reshape(hub_count, hub_stride, D)
    blocks = blocks.at[:, 0, :].add(directions)
    return jnp.clip(blocks.reshape(V, D), -5.0 * unit_scale, 5.0 * unit_scale).astype(jnp.bfloat16)


def draw_final_hidden(key, part):
    hub_stride, hub_count, directions = hub_layout(key)
    topics = jax.random.randint(jax.random.fold_in(key, 709), (TOKENS,), 0, hub_count)
    leaning = jax.random.uniform(jax.random.fold_in(key, 711), (TOKENS, 1), jnp.float32, 0.1, 0.45)
    base_rows = jax.random.truncated_normal(jax.random.fold_in(key, 713), -4.0, 4.0, (TOKENS, D), jnp.float32)
    pointed = jnp.take(directions, topics, axis=0) * math.sqrt(D)
    return jnp.clip(base_rows + leaning * pointed, -5.0, 5.0).astype(jnp.bfloat16)


def with_ends(entries, stream_key, low, high):
    dims = entries.shape
    spot = [jax.random.randint(jax.random.fold_in(stream_key, axis), (), 0, dims[axis]) for axis in range(len(dims))]
    entries = entries.at[tuple(spot)].set(low)
    longest = dims.index(max(dims))
    spot[longest] = (spot[longest] + 1) % dims[longest]
    return entries.at[tuple(spot)].set(high)


def cumulative_ranks(count, skew):
    loads = [(1 << 20) // math.isqrt(standing ** skew) + 1 for standing in range(1, count + 1)]
    width = 1 + sum(loads) // (1 << 30)
    return np.cumsum(np.array([max(1, weight // width) for weight in loads]))


def ranked_ids(key, dims, amount, skew):
    grid = cumulative_ranks(amount, skew)
    ticket = jax.random.randint(jax.random.fold_in(key, 1), dims, 0, int(grid[amount - 1]))
    standing = jnp.searchsorted(jnp.asarray(grid, jnp.int32), ticket, side="right")
    return jax.random.permutation(jax.random.fold_in(key, 2), amount)[standing].astype(jnp.int32)


def centred(stream_key, shape, scale, bound, dtype=jnp.bfloat16):
    values = jax.random.normal(stream_key, shape, jnp.float32) * scale
    return jnp.minimum(jnp.maximum(values, -bound), bound).astype(dtype)


def setup_inputs(seed: int = 0) -> dict:
    keys = jax.random.split(jax.random.key(seed), 8)
    input_ids = with_ends(ranked_ids(keys[0], (TOKENS,), V, 2), jax.random.fold_in(keys[0], 3), 0, V - 1).astype(jnp.int32)
    target_ids = with_ends(ranked_ids(keys[1], (TOKENS,), V, 2), jax.random.fold_in(keys[1], 3), 0, V - 1).astype(jnp.int32)
    loss_mask = with_ends((jax.random.randint(keys[2], (TOKENS,), 0, 8) < 7).astype(jnp.int32), jax.random.fold_in(keys[2], 1), 0, 1)
    final_hidden = draw_final_hidden(jax.random.fold_in(keys[7], 71), 0)
    norm_gain = jnp.clip(1.0 + 0.15 * jax.random.normal(keys[4], (D,), jnp.float32), 0.25, 1.75)
    embed_cotangent = centred(keys[5], (TOKENS, D), 0.01, 0.059814453)
    table = draw_table(jax.random.fold_in(keys[7], 71), 0)
    return dict(input_ids=input_ids, target_ids=target_ids, loss_mask=loss_mask, final_hidden=final_hidden, norm_gain=norm_gain, embed_cotangent=embed_cotangent, table=table)


EPSILON = 1e-06

def norm_backward(upstream, widened, inv_rms, norm_gain):
    scaled_up = upstream * norm_gain
    mean_dot = lax.optimization_barrier(jnp.mean(scaled_up * widened, axis=1, keepdims=True))
    gradient = inv_rms * scaled_up - widened * (inv_rms * inv_rms * inv_rms) * mean_dot
    gain_part = lax.optimization_barrier(jnp.sum(upstream * widened * inv_rms, axis=0))
    return (gradient.astype(jnp.bfloat16), gain_part)

def reference(input_ids, target_ids, loss_mask, final_hidden, norm_gain, embed_cotangent, table):
    block_count = N_DP * N_VOCAB
    block_rows = V // block_count
    embed_scale = math.sqrt(D)
    embedded = (jnp.take(table, input_ids, axis=0).astype(jnp.float32) * embed_scale).astype(jnp.bfloat16)
    widened = final_hidden.astype(jnp.float32)
    inv_rms = lax.rsqrt(lax.optimization_barrier(jnp.mean(widened * widened, axis=1, keepdims=True)) + EPSILON)
    normed = (widened * inv_rms * norm_gain).astype(jnp.bfloat16)
    blocks = table.reshape(block_count, block_rows, D)
    starts = (jnp.arange(block_count) * block_rows).astype(jnp.int32)

    def forward_block(rows_block):
        raw_logits = jnp.dot(normed, rows_block.T, preferred_element_type=jnp.float32)
        return SOFTCAP * jnp.tanh(raw_logits / SOFTCAP)
    capped = lax.map(forward_block, blocks)
    sum_exp = lax.optimization_barrier(jnp.sum(jnp.exp(capped), axis=(0, 2)))
    token_weight = loss_mask.astype(jnp.float32)
    cotangent_wide = embed_cotangent.astype(jnp.float32)

    def backward_block(carry, operands):
        upstream, picked = carry
        rows_block, start, capped_block = operands
        local_targets = (target_ids - start).astype(jnp.int32)
        target_hit = lax.broadcasted_iota(jnp.int32, capped_block.shape, 1) == local_targets[:, None]
        picked = picked + lax.optimization_barrier(jnp.sum(jnp.where(target_hit, capped_block, 0.0), axis=1))
        slope = token_weight[:, None] * (jnp.exp(capped_block) / sum_exp[:, None] - target_hit.astype(jnp.float32)) * (1.0 - (capped_block / SOFTCAP) ** 2)
        slope_low = slope.astype(jnp.bfloat16)
        upstream = upstream + jnp.dot(slope_low, rows_block, preferred_element_type=jnp.float32)
        head_part = lax.dot_general(slope_low, normed, (((0,), (0,)), ((), ())), preferred_element_type=jnp.float32)
        local_ids = (input_ids - start).astype(jnp.int32)
        inside = (local_ids >= 0) & (local_ids < block_rows)
        segment_ids = jnp.where(inside, local_ids, block_rows).astype(jnp.int32)
        embed_part = jax.ops.segment_sum(cotangent_wide, segment_ids, num_segments=block_rows + 1)[:block_rows] * embed_scale
        return ((upstream, picked), (head_part + embed_part).astype(jnp.bfloat16))
    initial = (jnp.zeros((TOKENS, D), jnp.float32), jnp.zeros((TOKENS,), jnp.float32))
    (upstream, picked), grad_blocks = lax.scan(backward_block, initial, (blocks, starts, capped))
    loss = jnp.sum(token_weight * (jnp.log(sum_exp) - picked)) / jnp.maximum(jnp.sum(token_weight), 1.0)
    grad_hidden, gain_grad = norm_backward(upstream, widened, inv_rms, norm_gain)
    table_grad = grad_blocks.reshape(V, D)
    return (embedded, loss, grad_hidden, gain_grad, table_grad)
```

```python
import functools
import math

import jax
import jax.numpy as jnp
from jax import lax
from jax.experimental import pallas as pl
from jax.experimental.pallas import tpu as pltpu
from jax.sharding import PartitionSpec as P

SOFTCAP = 30
EPSILON = 1e-06
LANES = 128


def enter(count, others):
    barrier = pltpu.get_barrier_semaphore()
    for other in others:
        pl.semaphore_signal(barrier, inc=1, device_id={"vocab": other})
    pl.semaphore_wait(barrier, count)


def stats_kernel(n, x_ref, out_ref, slots, mine, send_sem, recv_sem):
    me = lax.axis_index("vocab")
    enter(n - 1, [lax.rem(me + o, n) for o in range(1, n)])
    mine[...] = x_ref[...]

    def copy(o):
        return pltpu.make_async_remote_copy(
            src_ref=mine,
            dst_ref=slots.at[me],
            send_sem=send_sem.at[o],
            recv_sem=recv_sem.at[o],
            device_id={"vocab": lax.rem(me + o, n)},
        )

    def arrival(o):
        return pltpu.make_async_remote_copy(
            src_ref=mine,
            dst_ref=slots.at[lax.rem(me - o + n, n)],
            send_sem=send_sem.at[o],
            recv_sem=recv_sem.at[o],
            device_id={"vocab": lax.rem(me + o, n)},
        )

    for o in range(1, n):
        copy(o).start()
    slots[me] = x_ref[...]
    for o in range(1, n):
        arrival(o).wait_recv()
    total = slots[0]
    for source in range(1, n):
        total = total + slots[source]
    out_ref[...] = total
    for o in range(1, n):
        copy(o).wait_send()


def exchange_stats(n, values):
    if n == 1:
        return values
    return pl.pallas_call(
        functools.partial(stats_kernel, n),
        out_shape=jax.ShapeDtypeStruct(values.shape, values.dtype),
        in_specs=[pl.BlockSpec(memory_space=pltpu.VMEM)],
        out_specs=pl.BlockSpec(memory_space=pltpu.VMEM),
        scratch_shapes=[
            pltpu.VMEM((n,) + values.shape, values.dtype),
            pltpu.VMEM(values.shape, values.dtype),
            pltpu.SemaphoreType.DMA((n,)),
            pltpu.SemaphoreType.DMA((n,)),
        ],
        compiler_params=pltpu.CompilerParams(collective_id=1, has_side_effects=True),
    )(values)


def stream_plan(levels, width):
    rest = [g for g in ([1], [2], list(range(3, levels))) if g and g[-1] < levels]
    shares = [11, 10, 7]
    tiles = width // LANES
    plans, start = [], 0
    for i in range(max(1, len(rest))):
        order = [0] + [b for g in rest[i:] + rest[:i] for b in g]
        last = i == max(1, len(rest)) - 1
        stop = tiles if last else start + tiles * shares[i] // sum(shares)
        plans.append((slice(start * LANES, stop * LANES), order))
        start = stop
    return plans


def hidden_kernel(levels, plans, *refs):
    count = len(plans)
    up_ref, found_ref, hidden_ref, gain_ref, grad_ref, emb_ref, gain_out_ref = refs[:7]
    scratch = list(refs[7:])
    acc = [scratch.pop(0) for _ in plans]
    got_wide = [scratch.pop(0) for _ in plans]
    low = [scratch.pop(0) for _ in plans]
    got = [scratch.pop(0) for _ in plans]
    whole = [scratch.pop(0) for _ in plans]
    facc = [scratch.pop(0) for _ in plans]
    fgot = [scratch.pop(0) for _ in plans]
    fwhole = [scratch.pop(0) for _ in plans]
    gains, gain_got, send_sem, recv_sem = scratch
    n = 2**levels
    width = up_ref.shape[2]
    me = lax.axis_index("vocab")
    bits = [lax.rem(me // 2**b, 2) for b in range(levels)]
    partner = [me + (1 - 2 * bits[b]) * 2**b for b in range(levels)]
    enter(levels, partner)

    def chunk_of(position, order):
        return sum(
            lax.rem(position // 2 ** (levels - 1 - j), 2) * 2 ** order[j] for j in range(levels)
        )

    def base_of(order, known):
        return sum([bits[order[j]] * 2 ** (levels - 1 - j) for j in range(known)], 0)

    def each(size, step):
        def wrapped(i, carry):
            step(i)
            return carry

        lax.fori_loop(0, size, wrapped, 0, unroll=min(size, 4))

    def remote(src, dst, flow, stage, bit):
        return pltpu.make_async_remote_copy(
            src_ref=src,
            dst_ref=dst,
            send_sem=send_sem.at[flow, stage],
            recv_sem=recv_sem.at[flow, stage],
            device_id={"vocab": partner[bit]},
        )

    for k in range(levels):
        size = 2 ** (levels - 1 - k)
        wide = k not in (1, 2)
        sent, landed = (acc, got_wide) if wide else (low, got)
        copies = []
        for s, (columns, order) in enumerate(plans):
            bit = order[k]
            base = base_of(order, k)
            keep = base + bits[bit] * size
            give = base + (1 - bits[bit]) * size

            def prepare(i, s=s, order=order, columns=columns, give=give, keep=keep):
                if k == 0:
                    out_chunk = chunk_of(give + i, order)
                    acc[s][give + i] = up_ref[out_chunk, :, columns]
                    facc[s][give + i] = found_ref[out_chunk, :, columns].astype(jnp.bfloat16)
                elif not wide:
                    low[s][give + i] = acc[s][give + i].astype(jnp.bfloat16)

            each(size, prepare)
            arrived = pl.ds(size, size)
            first = remote(
                sent[s].at[pl.ds(give, size)], landed[s].at[arrived], s, k, bit
            )
            second = remote(
                facc[s].at[pl.ds(give, size)], fgot[s].at[arrived], count + s, k, bit
            )
            first.start()
            second.start()
            copies.append((first, second, keep))
        for s, (columns, order) in enumerate(plans):
            first, second, keep = copies[s]
            first.wait_recv()

            def add(i, s=s, order=order, columns=columns, keep=keep, landed=landed):
                arrived = landed[s][size + i].astype(jnp.float32)
                if k == 0:
                    acc[s][keep + i] = up_ref[chunk_of(keep + i, order), :, columns] + arrived
                else:
                    acc[s][keep + i] = acc[s][keep + i] + arrived

            each(size, add)
            second.wait_recv()

            def merge(i, s=s, order=order, columns=columns, keep=keep):
                arrived = fgot[s][size + i]
                if k == 0:
                    own = found_ref[chunk_of(keep + i, order), :, columns].astype(jnp.bfloat16)
                else:
                    own = facc[s][keep + i]
                facc[s][keep + i] = own + arrived

            each(size, merge)
        for first, second, _ in copies:
            first.wait_send()
            second.wait_send()

    full = hidden_ref[...]
    inv = lax.rsqrt(jnp.sum(full * full, axis=1, keepdims=True) / width + EPSILON)
    own = [base_of(order, levels) for _, order in plans]
    dot = sum(
        jnp.sum(
            acc[s][own[s]] * gain_ref[:, columns] * full[:, columns], axis=1, keepdims=True
        )
        for s, (columns, _) in enumerate(plans)
    )
    mean_dot = dot / width
    gains[0] = jnp.zeros(gains.shape[1:], jnp.float32)
    for s, (columns, _) in enumerate(plans):
        upstream = acc[s][own[s]]
        wide = full[:, columns]
        gradient = inv * (upstream * gain_ref[:, columns]) - wide * (inv * inv * inv) * mean_dot
        whole[s][own[s]] = gradient.astype(jnp.bfloat16)
        fwhole[s][own[s]] = facc[s][own[s]]
        part = jnp.sum(upstream * wide * inv, axis=0, keepdims=True)
        for j in range(columns.start // LANES, columns.stop // LANES):
            lanes = slice(j * LANES - columns.start, (j + 1) * LANES - columns.start)
            gains[0, j : j + 1, :] = part[:, lanes]

    for t in range(levels):
        size = 2**t
        stage = levels + t
        copies = []
        for s, (columns, order) in enumerate(plans):
            bit = order[levels - 1 - t]
            base = base_of(order, levels - t)
            block = pl.ds(base, size)
            copies.append(remote(whole[s].at[block], whole[s].at[block], s, stage, bit))
            copies.append(
                remote(fwhole[s].at[block], fwhole[s].at[block], count + s, stage, bit)
            )
        copies.append(remote(gains.at[t], gain_got.at[t], 2 * count, stage, t))
        for copy in copies:
            copy.start()
        for copy in copies:
            copy.wait_recv()
        gains[t + 1] = gains[t] + gain_got[t]
        for copy in copies:
            copy.wait_send()
    gain_out_ref[...] = gains[levels]
    for s, (columns, order) in enumerate(plans):

        def place(i, s=s, order=order, columns=columns):
            pair = chunk_of(i, order) // 2
            for out_ref, source in ((grad_ref, whole[s]), (emb_ref, fwhole[s])):
                both = [source[p].astype(jnp.float32) for p in (i, i + n // 2)]
                out_ref[pair, :, columns] = jnp.concatenate(both, axis=0).astype(jnp.bfloat16)

        each(n // 2, place)


def reduce_hidden(n, upstream, found, final_hidden, norm_gain):
    tokens, width = upstream.shape
    levels = n.bit_length() - 1
    share = tokens // n
    plans = stream_plan(levels, width)
    sizes = [(n, share, columns.stop - columns.start) for columns, _ in plans]
    narrow = [pltpu.VMEM((n + 1,) + size[1:], jnp.bfloat16) for size in sizes]
    first = lax.axis_index("vocab") * share
    own_hidden = lax.dynamic_slice_in_dim(final_hidden, first, share, 0).astype(jnp.float32)
    lines = -(-width // (8 * LANES)) * 8
    pairs = (n // 2, 2 * share, width)
    blocks = (n, share, width)
    flows = 2 * len(plans) + 1
    vmem = pl.BlockSpec(memory_space=pltpu.VMEM)
    grad, emb, gain = pl.pallas_call(
        functools.partial(hidden_kernel, levels, plans),
        out_shape=(
            jax.ShapeDtypeStruct(pairs, jnp.bfloat16),
            jax.ShapeDtypeStruct(pairs, jnp.bfloat16),
            jax.ShapeDtypeStruct((lines, LANES), jnp.float32),
        ),
        in_specs=[vmem] * 4,
        out_specs=(vmem, vmem, vmem),
        scratch_shapes=[pltpu.VMEM(size, jnp.float32) for size in sizes] * 2
        + narrow * 6
        + [
            pltpu.VMEM((levels + 1, lines, LANES), jnp.float32),
            pltpu.VMEM((levels, lines, LANES), jnp.float32),
            pltpu.SemaphoreType.DMA((flows, 2 * levels)),
            pltpu.SemaphoreType.DMA((flows, 2 * levels)),
        ],
        compiler_params=pltpu.CompilerParams(
            collective_id=2, has_side_effects=True, vmem_limit_bytes=48 * 1024 * 1024
        ),
    )(
        upstream.reshape(blocks),
        found.reshape(blocks),
        own_hidden,
        jnp.broadcast_to(norm_gain, (share, width)),
    )
    return grad.reshape(tokens, width), emb.reshape(tokens, width), gain.reshape(-1)[:width]


def table_kernel(scale, step, ids_ref, slope_ref, normed_ref, cotangent_ref, out_ref):
    rows, tokens = slope_ref.shape
    row_ids = lax.broadcasted_iota(jnp.int32, (rows, tokens), 0) + pl.program_id(0) * rows
    hit = (row_ids == ids_ref[...]).astype(jnp.float32).astype(jnp.bfloat16)

    def tile(j, carry):
        columns = pl.ds(pl.multiple_of(j * step, step), step)
        head = jnp.dot(
            slope_ref[...], normed_ref[:, columns], preferred_element_type=jnp.float32
        )
        embed = jnp.dot(hit, cotangent_ref[:, columns], preferred_element_type=jnp.float32)
        out_ref[:, columns] = (head + embed * scale).astype(jnp.bfloat16)
        return carry

    lax.fori_loop(0, out_ref.shape[1] // step, tile, 0)


def table_gradient(scale, local_ids, slope, normed, cotangent):
    row_count, tokens = slope.shape
    width = normed.shape[1]
    block = max(b for b in range(16, 401, 16) if row_count % b == 0)
    step = 512 if width % 512 == 0 else LANES
    vmem = pl.BlockSpec(memory_space=pltpu.VMEM)
    return pl.pallas_call(
        functools.partial(table_kernel, scale, step),
        grid=(row_count // block,),
        out_shape=jax.ShapeDtypeStruct((row_count, width), jnp.bfloat16),
        in_specs=[vmem, pl.BlockSpec((block, tokens), lambda i: (i, 0)), vmem, vmem],
        out_specs=pl.BlockSpec((block, width), lambda i: (i, 0)),
        compiler_params=pltpu.CompilerParams(vmem_limit_bytes=48 * 1024 * 1024),
        cost_estimate=pl.CostEstimate(
            flops=4 * row_count * tokens * width,
            bytes_accessed=2 * row_count * width,
            transcendentals=0,
        ),
    )(local_ids.reshape(1, tokens), slope, normed, cotangent)


def body(input_ids, target_ids, loss_mask, final_hidden, norm_gain, embed_cotangent, table):
    row_count, width = table.shape
    embed_scale = math.sqrt(width)
    n = lax.axis_size("vocab")
    first_row = lax.axis_index(("dp", "vocab")) * row_count
    every_id, every_target, every_mask = (
        lax.all_gather(a, "dp", axis=0, tiled=True) for a in (input_ids, target_ids, loss_mask)
    )
    tokens = every_id.shape[0]
    widened = final_hidden.astype(jnp.float32)
    inv_rms = lax.rsqrt(jnp.mean(widened * widened, axis=1, keepdims=True) + EPSILON)
    normed = (widened * inv_rms * norm_gain).astype(jnp.bfloat16)
    normed_all, cotangent_all = (
        lax.all_gather(a, "dp", axis=0, tiled=True) for a in (normed, embed_cotangent)
    )
    raw_logits = lax.dot_general(
        table, normed_all, (((1,), (1,)), ((), ())), preferred_element_type=jnp.float32
    )
    capped = SOFTCAP * jnp.tanh(raw_logits / SOFTCAP)
    row_ids = lax.broadcasted_iota(jnp.int32, capped.shape, 0) + first_row
    target_hit = row_ids == every_target[None, :]
    token_weight = every_mask.astype(jnp.float32)
    sums = jnp.stack(
        [jnp.sum(jnp.exp(capped), axis=0), jnp.sum(jnp.where(target_hit, capped, 0.0), axis=0)]
    )
    sums = exchange_stats(n, sums.reshape(-1, LANES)).reshape(2, tokens)
    sum_exp, target_logit = lax.psum(sums, "dp")
    loss = jnp.sum(token_weight * (jnp.log(sum_exp) - target_logit)) / jnp.maximum(
        jnp.sum(token_weight), 1.0
    )
    slope = (
        token_weight[None, :]
        * (jnp.exp(capped) / sum_exp[None, :] - target_hit.astype(jnp.float32))
        * (1.0 - (capped / SOFTCAP) ** 2)
    ).astype(jnp.bfloat16)
    slope = lax.optimization_barrier(slope)
    id_rows = lax.broadcasted_iota(jnp.int32, (tokens, row_count), 1) + first_row
    id_hit = lax.optimization_barrier((id_rows == every_id[:, None]).astype(jnp.bfloat16))
    upstream = lax.dot_general(
        slope, table, (((0,), (0,)), ((), ())), preferred_element_type=jnp.float32
    )
    found = lax.dot_general(
        id_hit, table, (((1,), (0,)), ((), ())), preferred_element_type=jnp.float32
    )
    if lax.axis_size("dp") > 1:
        upstream = lax.psum_scatter(upstream, "dp", scatter_dimension=0, tiled=True)
        found = lax.psum_scatter(found.astype(jnp.bfloat16), "dp", scatter_dimension=0, tiled=True).astype(jnp.float32)
    grad_hidden, rows, gain_part = reduce_hidden(n, upstream, found, final_hidden, norm_gain)
    embedded = (rows.astype(jnp.float32) * embed_scale).astype(jnp.bfloat16)
    gain_grad = lax.psum(gain_part, "dp")
    table_grad = table_gradient(
        embed_scale, every_id - first_row, slope, normed_all, cotangent_all
    )
    return (embedded, loss, grad_hidden, gain_grad, table_grad)


def solution(mesh):
    placed = (
        P("dp"),
        P("dp"),
        P("dp"),
        P("dp", None),
        P(),
        P("dp", None),
        P(("dp", "vocab"), None),
    )
    return jax.shard_map(
        body,
        mesh=mesh,
        in_specs=placed,
        out_specs=(P("dp", None), P(), P("dp", None), P(), P(("dp", "vocab"), None)),
        check_vma=False,
    )
```

```python
import functools
import math

import jax
import jax.numpy as jnp
from jax import lax
from jax.experimental import pallas as pl
from jax.experimental.pallas import tpu as pltpu
from jax.sharding import PartitionSpec as P

SOFTCAP = 30
EPSILON = 1e-06
LANES = 128


def enter(count, others):
    barrier = pltpu.get_barrier_semaphore()
    for other in others:
        pl.semaphore_signal(barrier, inc=1, device_id={"vocab": other})
    pl.semaphore_wait(barrier, count)


def stats_kernel(n, x_ref, out_ref, slots, mine, send_sem, recv_sem):
    me = lax.axis_index("vocab")
    enter(n - 1, [lax.rem(me + o, n) for o in range(1, n)])
    mine[...] = x_ref[...]

    def copy(o):
        return pltpu.make_async_remote_copy(
            src_ref=mine,
            dst_ref=slots.at[me],
            send_sem=send_sem.at[o],
            recv_sem=recv_sem.at[o],
            device_id={"vocab": lax.rem(me + o, n)},
        )

    def arrival(o):
        return pltpu.make_async_remote_copy(
            src_ref=mine,
            dst_ref=slots.at[lax.rem(me - o + n, n)],
            send_sem=send_sem.at[o],
            recv_sem=recv_sem.at[o],
            device_id={"vocab": lax.rem(me + o, n)},
        )

    for o in range(1, n):
        copy(o).start()
    slots[me] = x_ref[...]
    for o in range(1, n):
        arrival(o).wait_recv()
    total = slots[0]
    for source in range(1, n):
        total = total + slots[source]
    out_ref[...] = total
    for o in range(1, n):
        copy(o).wait_send()


def exchange_stats(n, values):
    if n == 1:
        return values
    return pl.pallas_call(
        functools.partial(stats_kernel, n),
        out_shape=jax.ShapeDtypeStruct(values.shape, values.dtype),
        in_specs=[pl.BlockSpec(memory_space=pltpu.VMEM)],
        out_specs=pl.BlockSpec(memory_space=pltpu.VMEM),
        scratch_shapes=[
            pltpu.VMEM((n,) + values.shape, values.dtype),
            pltpu.VMEM(values.shape, values.dtype),
            pltpu.SemaphoreType.DMA((n,)),
            pltpu.SemaphoreType.DMA((n,)),
        ],
        compiler_params=pltpu.CompilerParams(collective_id=1, has_side_effects=True),
        cost_estimate=pl.CostEstimate(flops=0, bytes_accessed=2**25, transcendentals=0),
    )(values)


def stream_plan(levels, width):
    rest = [g for g in ([1], [2], list(range(3, levels))) if g and g[-1] < levels]
    shares = [11, 10, 7]
    tiles = width // LANES
    plans, start = [], 0
    for i in range(max(1, len(rest))):
        order = [0] + [b for g in rest[i:] + rest[:i] for b in g]
        last = i == max(1, len(rest)) - 1
        stop = tiles if last else start + tiles * shares[i] // sum(shares)
        plans.append((slice(start * LANES, stop * LANES), order))
        start = stop
    return plans


def hidden_kernel(levels, plans, *refs):
    count = len(plans)
    up_ref, found_ref, hidden_ref, gain_ref, grad_ref, emb_ref, gain_out_ref = refs[:7]
    scratch = list(refs[7:])
    acc = [scratch.pop(0) for _ in plans]
    got_wide = [scratch.pop(0) for _ in plans]
    low = [scratch.pop(0) for _ in plans]
    got = [scratch.pop(0) for _ in plans]
    whole = [scratch.pop(0) for _ in plans]
    fwhole = [scratch.pop(0) for _ in plans]
    gains, gain_got, send_sem, recv_sem = scratch
    n = 2**levels
    width = up_ref.shape[2]
    me = lax.axis_index("vocab")
    bits = [lax.rem(me // 2**b, 2) for b in range(levels)]
    partner = [me + (1 - 2 * bits[b]) * 2**b for b in range(levels)]
    enter(levels, partner)

    def chunk_of(position, order):
        return sum(
            lax.rem(position // 2 ** (levels - 1 - j), 2) * 2 ** order[j] for j in range(levels)
        )

    def base_of(order, known):
        return sum([bits[order[j]] * 2 ** (levels - 1 - j) for j in range(known)], 0)

    def each(size, step):
        def wrapped(i, carry):
            step(i)
            return carry

        lax.fori_loop(0, size, wrapped, 0, unroll=min(size, 4))

    def remote(src, dst, flow, stage, bit):
        return pltpu.make_async_remote_copy(
            src_ref=src,
            dst_ref=dst,
            send_sem=send_sem.at[flow, stage],
            recv_sem=recv_sem.at[flow, stage],
            device_id={"vocab": partner[bit]},
        )

    def gather_copy(buffers, flow, s, t):
        order = plans[s][1]
        block = pl.ds(base_of(order, levels - t), 2**t)
        bit = order[levels - 1 - t]
        stage = levels + t
        return remote(buffers[s].at[block], buffers[s].at[block], flow + s, stage, bit)

    for s, (columns, order) in enumerate(plans):
        fwhole[s][base_of(order, levels)] = found_ref[:, columns].astype(jnp.bfloat16)

    for k in range(levels):
        size = 2 ** (levels - 1 - k)
        wide = k not in (1, 2)
        sent, landed = (acc, got_wide) if wide else (low, got)
        copies = []
        for s, (columns, order) in enumerate(plans):
            bit = order[k]
            base = base_of(order, k)
            keep = base + bits[bit] * size
            give = base + (1 - bits[bit]) * size

            def prepare(i, s=s, order=order, columns=columns, give=give, keep=keep):
                if k == 0:
                    out_chunk = chunk_of(give + i, order)
                    acc[s][give + i] = up_ref[out_chunk, :, columns]
                elif not wide:
                    low[s][give + i] = acc[s][give + i].astype(jnp.bfloat16)

            each(size, prepare)
            arrived = pl.ds(size, size)
            first = remote(
                sent[s].at[pl.ds(give, size)], landed[s].at[arrived], s, k, bit
            )
            first.start()
            second = gather_copy(fwhole, count, s, k)
            second.start()
            copies.append((first, second, keep))
        for s, (columns, order) in enumerate(plans):
            first, second, keep = copies[s]
            first.wait_recv()

            def add(i, s=s, order=order, columns=columns, keep=keep, landed=landed):
                arrived = landed[s][size + i].astype(jnp.float32)
                if k == 0:
                    acc[s][keep + i] = up_ref[chunk_of(keep + i, order), :, columns] + arrived
                else:
                    acc[s][keep + i] = acc[s][keep + i] + arrived

            each(size, add)
            second.wait_recv()
        for first, second, _ in copies:
            first.wait_send()
            second.wait_send()

    full = hidden_ref[...]
    inv = lax.rsqrt(jnp.sum(full * full, axis=1, keepdims=True) / width + EPSILON)
    own = [base_of(order, levels) for _, order in plans]
    dot = sum(
        jnp.sum(
            acc[s][own[s]] * gain_ref[:, columns] * full[:, columns], axis=1, keepdims=True
        )
        for s, (columns, _) in enumerate(plans)
    )
    mean_dot = dot / width
    gains[0] = jnp.zeros(gains.shape[1:], jnp.float32)
    for s, (columns, _) in enumerate(plans):
        upstream = acc[s][own[s]]
        wide = full[:, columns]
        gradient = inv * (upstream * gain_ref[:, columns]) - wide * (inv * inv * inv) * mean_dot
        whole[s][own[s]] = gradient.astype(jnp.bfloat16)
        part = jnp.sum(upstream * wide * inv, axis=0, keepdims=True)
        for j in range(columns.start // LANES, columns.stop // LANES):
            lanes = slice(j * LANES - columns.start, (j + 1) * LANES - columns.start)
            gains[0, j : j + 1, :] = part[:, lanes]

    for t in range(levels):
        copies = [gather_copy(whole, 0, s, t) for s in range(count)]
        copies.append(remote(gains.at[t], gain_got.at[t], 2 * count, levels + t, t))
        for copy in copies:
            copy.start()
        for copy in copies:
            copy.wait_recv()
        gains[t + 1] = gains[t] + gain_got[t]
        for copy in copies:
            copy.wait_send()
    gain_out_ref[...] = gains[levels]
    for s, (columns, order) in enumerate(plans):

        def place(i, s=s, order=order, columns=columns):
            pair = chunk_of(i, order) // 2
            for out_ref, source in ((grad_ref, whole[s]), (emb_ref, fwhole[s])):
                both = [source[p].astype(jnp.float32) for p in (i, i + n // 2)]
                out_ref[pair, :, columns] = jnp.concatenate(both, axis=0).astype(jnp.bfloat16)

        each(n // 2, place)


def reduce_hidden(n, upstream, found, final_hidden, norm_gain):
    tokens, width = upstream.shape
    levels = n.bit_length() - 1
    share = tokens // n
    plans = stream_plan(levels, width)
    sizes = [(n, share, columns.stop - columns.start) for columns, _ in plans]
    narrow = [pltpu.VMEM((n + 1,) + size[1:], jnp.bfloat16) for size in sizes]
    first = lax.axis_index("vocab") * share
    own_hidden = lax.dynamic_slice_in_dim(final_hidden, first, share, 0).astype(jnp.float32)
    lines = -(-width // (8 * LANES)) * 8
    pairs = (n // 2, 2 * share, width)
    blocks = (n, share, width)
    flows = 2 * len(plans) + 1
    vmem = pl.BlockSpec(memory_space=pltpu.VMEM)
    grad, emb, gain = pl.pallas_call(
        functools.partial(hidden_kernel, levels, plans),
        out_shape=(
            jax.ShapeDtypeStruct(pairs, jnp.bfloat16),
            jax.ShapeDtypeStruct(pairs, jnp.bfloat16),
            jax.ShapeDtypeStruct((lines, LANES), jnp.float32),
        ),
        in_specs=[vmem] * 4,
        out_specs=(vmem, vmem, vmem),
        scratch_shapes=[pltpu.VMEM(size, jnp.float32) for size in sizes] * 2
        + narrow * 4
        + [
            pltpu.VMEM((levels + 1, lines, LANES), jnp.float32),
            pltpu.VMEM((levels, lines, LANES), jnp.float32),
            pltpu.SemaphoreType.DMA((flows, 2 * levels)),
            pltpu.SemaphoreType.DMA((flows, 2 * levels)),
        ],
        compiler_params=pltpu.CompilerParams(
            collective_id=2, has_side_effects=True, vmem_limit_bytes=48 * 1024 * 1024
        ),
    )(
        upstream.reshape(blocks),
        found,
        own_hidden,
        jnp.broadcast_to(norm_gain, (share, width)),
    )
    return grad.reshape(tokens, width), emb.reshape(tokens, width), gain.reshape(-1)[:width]


def halving_sum(n, values):
    me = lax.axis_index("vocab")
    for b in range(n.bit_length() - 1):
        bit = lax.rem(me // 2**b, 2)
        half = values.shape[0] // 2
        give = lax.dynamic_slice_in_dim(values, (1 - bit) * half, half, 0)
        keep = lax.dynamic_slice_in_dim(values, bit * half, half, 0)
        pairs = [(d, d ^ 2**b) for d in range(n)]
        arrived = lax.ppermute(give.astype(jnp.bfloat16), "vocab", pairs)
        values = keep.astype(jnp.float32) + arrived.astype(jnp.float32)
    return values


def reversed_bits(n, values):
    levels = n.bit_length() - 1
    split = values.reshape((2,) * levels + (values.shape[0] // n,))
    return split.transpose(tuple(reversed(range(levels))) + (levels,)).reshape(values.shape)


def table_kernel(scale, step, ids_ref, slope_ref, normed_ref, cotangent_ref, out_ref):
    rows, tokens = slope_ref.shape
    row_ids = lax.broadcasted_iota(jnp.int32, (rows, tokens), 0) + pl.program_id(0) * rows
    hit = (row_ids == ids_ref[...]).astype(jnp.float32).astype(jnp.bfloat16)

    def tile(j, carry):
        columns = pl.ds(pl.multiple_of(j * step, step), step)
        head = jnp.dot(
            slope_ref[...], normed_ref[:, columns], preferred_element_type=jnp.float32
        )
        embed = jnp.dot(hit, cotangent_ref[:, columns], preferred_element_type=jnp.float32)
        out_ref[:, columns] = (head + embed * scale).astype(jnp.bfloat16)
        return carry

    lax.fori_loop(0, out_ref.shape[1] // step, tile, 0)


def table_gradient(scale, local_ids, slope, normed, cotangent):
    row_count, tokens = slope.shape
    width = normed.shape[1]
    block = max(b for b in range(16, 401, 16) if row_count % b == 0)
    step = 512 if width % 512 == 0 else LANES
    vmem = pl.BlockSpec(memory_space=pltpu.VMEM)
    return pl.pallas_call(
        functools.partial(table_kernel, scale, step),
        grid=(row_count // block,),
        out_shape=jax.ShapeDtypeStruct((row_count, width), jnp.bfloat16),
        in_specs=[vmem, pl.BlockSpec((block, tokens), lambda i: (i, 0)), vmem, vmem],
        out_specs=pl.BlockSpec((block, width), lambda i: (i, 0)),
        compiler_params=pltpu.CompilerParams(vmem_limit_bytes=48 * 1024 * 1024),
        cost_estimate=pl.CostEstimate(
            flops=4 * row_count * tokens * width,
            bytes_accessed=2 * row_count * width,
            transcendentals=0,
        ),
    )(local_ids.reshape(1, tokens), slope, normed, cotangent)


def body(input_ids, target_ids, loss_mask, final_hidden, norm_gain, embed_cotangent, table):
    row_count, width = table.shape
    embed_scale = math.sqrt(width)
    n = lax.axis_size("vocab")
    first_row = lax.axis_index(("dp", "vocab")) * row_count
    every_id, every_target, every_mask = (
        lax.all_gather(a, "dp", axis=0, tiled=True) for a in (input_ids, target_ids, loss_mask)
    )
    tokens = every_id.shape[0]
    widened = final_hidden.astype(jnp.float32)
    inv_rms = lax.rsqrt(jnp.mean(widened * widened, axis=1, keepdims=True) + EPSILON)
    normed = (widened * inv_rms * norm_gain).astype(jnp.bfloat16)
    normed_all, cotangent_all = (
        lax.all_gather(a, "dp", axis=0, tiled=True) for a in (normed, embed_cotangent)
    )
    share = tokens // lax.axis_size("dp") // n
    groups = every_id.reshape(-1, n * share)
    sorted_id = jax.vmap(functools.partial(reversed_bits, n))(groups).reshape(-1)
    id_rows = lax.broadcasted_iota(jnp.int32, (tokens, row_count), 1) + first_row
    id_hit = lax.optimization_barrier((id_rows == sorted_id[:, None]).astype(jnp.bfloat16))
    found = lax.dot_general(
        id_hit, table, (((1,), (0,)), ((), ())), preferred_element_type=jnp.float32
    ).astype(jnp.bfloat16)
    if lax.axis_size("dp") > 1:
        found = lax.psum_scatter(found, "dp", scatter_dimension=0, tiled=True)
    found = halving_sum(n, found)
    raw_logits = lax.dot_general(
        table, normed_all, (((1,), (1,)), ((), ())), preferred_element_type=jnp.float32
    )
    capped = SOFTCAP * jnp.tanh(raw_logits / SOFTCAP)
    row_ids = lax.broadcasted_iota(jnp.int32, capped.shape, 0) + first_row
    target_hit = row_ids == every_target[None, :]
    token_weight = every_mask.astype(jnp.float32)
    sums = jnp.stack(
        [jnp.sum(jnp.exp(capped), axis=0), jnp.sum(jnp.where(target_hit, capped, 0.0), axis=0)]
    )
    sums = exchange_stats(n, sums.reshape(-1, LANES)).reshape(2, tokens)
    sum_exp, target_logit = lax.psum(sums, "dp")
    loss = jnp.sum(token_weight * (jnp.log(sum_exp) - target_logit)) / jnp.maximum(
        jnp.sum(token_weight), 1.0
    )
    slope = (
        token_weight[None, :]
        * (jnp.exp(capped) / sum_exp[None, :] - target_hit.astype(jnp.float32))
        * (1.0 - (capped / SOFTCAP) ** 2)
    ).astype(jnp.bfloat16)
    slope = lax.optimization_barrier(slope)
    upstream = lax.dot_general(
        slope, table, (((0,), (0,)), ((), ())), preferred_element_type=jnp.float32
    )
    if lax.axis_size("dp") > 1:
        upstream = lax.psum_scatter(upstream, "dp", scatter_dimension=0, tiled=True)
    grad_hidden, rows, gain_part = reduce_hidden(n, upstream, found, final_hidden, norm_gain)
    embedded = (rows.astype(jnp.float32) * embed_scale).astype(jnp.bfloat16)
    gain_grad = lax.psum(gain_part, "dp")
    table_grad = table_gradient(
        embed_scale, every_id - first_row, slope, normed_all, cotangent_all
    )
    return (embedded, loss, grad_hidden, gain_grad, table_grad)


def solution(mesh):
    placed = (
        P("dp"),
        P("dp"),
        P("dp"),
        P("dp", None),
        P(),
        P("dp", None),
        P(("dp", "vocab"), None),
    )
    return jax.shard_map(
        body,
        mesh=mesh,
        in_specs=placed,
        out_specs=(P("dp", None), P(), P("dp", None), P(), P(("dp", "vocab"), None)),
        check_vma=False,
    )
```
